1024 devices in a mesh: dp: 128 (over z, y, core), tensor: 8 (over x).
Axes of the slice: x: 8, y: 8, z: 8, core: 2. Of those that a mesh axis runs over, the one named last changes fastest.
Arguments:
- grads: bfloat16 [128, 2, 4096, 1024], P('dp', None, None, 'tensor'), may hold values from -480 to 480
- master: float32 [2, 4096, 1024], P(None, 'dp', 'tensor'), may hold values from -0.09375 to 0.09375
- moment: float32 [2, 4096, 1024], P(None, 'dp', 'tensor'), may hold values from -0.06 to 0.06
- v_heads: float32 [8], P('tensor'), may hold values from 0.0001 to 0.001
- v_neurons: float32 [1024], P('tensor'), may hold values from 0.0001 to 0.001
Outputs:
- params: bfloat16 [2, 4096, 1024], P(None, None, 'tensor')
- new_master: float32 [2, 4096, 1024], P(None, 'dp', 'tensor')
- new_moment: float32 [2, 4096, 1024], P(None, 'dp', 'tensor')
- new_heads: float32 [8], P('tensor')
- new_neurons: float32 [1024], P('tensor')
The draws below stay inside these ranges and needn't reach their ends.
All inputs are finite; a program needn't handle non-finite values.
Results may differ from the reference program's by a relative error of at most 0.001.
Values may be sent and summed in bfloat16 or wider, within the bound.
No kernel may reach another device: no remote copies, remote signals or barrier semaphores. Data moves between devices by JAX's collectives and lax.ppermute only.
A program may use at most 32 MiB of HBM per device.

```python
import math
import jax
import jax.numpy as jnp
from jax import lax

DIN = 4096
KVH = 8
HEAD = 128
STEP = 2
N_DP = 128


def draw_grads(key, part):
    columns = KVH * HEAD
    keys = jax.random.split(key, 3)
    row_rand = jnp.exp(jax.random.uniform(keys[0], (DIN,), jnp.float32, 0.0, math.log(10.0)))
    rows = jnp.arange(DIN, dtype=jnp.float32) / DIN
    row_scale = row_rand * (1.0 + 2.0 * rows)
    col_scale = 1.0 + 2.0 * jnp.arange(columns, dtype=jnp.float32) / columns
    order = jax.random.permutation(keys[1], N_DP)
    row_block = jnp.arange(DIN) // (DIN // N_DP)
    spike = jnp.where(row_block[None, :] == order[:, None], 4.0, 1.0)
    shape = (N_DP, 2, DIN, columns)
    base = jnp.clip(jax.random.normal(keys[2], shape, jnp.float32), -4.0, 4.0)
    values = base * spike[:, None, :, None] * row_scale[None, None, :, None] * col_scale[None, None, None, :]
    values = jnp.clip(values, -480.0, 480.0)
    return values.astype(jnp.bfloat16)


def level_of(stream_key, extent, shards, smallest, top_value):
    loudness = 1.0
    for dim, parts in shards:
        steps = jax.random.uniform(jax.random.fold_in(jax.random.fold_in(stream_key, 6), dim), (parts,), jnp.float32, smallest / len(shards), top_value / len(shards))
        loudness = loudness * jnp.repeat(jnp.exp(steps), extent[dim] // parts).reshape((-1,) + (1,) * (len(extent) - 1 - dim))
    return loudness


def bell_draw(own_key, dims, width, limit, shards=(), held_as=jnp.bfloat16):
    result = jax.random.normal(own_key, dims, jnp.float32) * width
    if len(shards) > 0:
        result = level_of(own_key, dims, shards, -0.22, 0.18) * result
    return jnp.clip(result, min=-limit, max=limit).astype(held_as)


def setup_inputs(seed: int = 0) -> dict:
    streams_of = jax.random.split(jax.random.key(seed), 6)
    return {
        "grads": draw_grads(jax.random.fold_in(streams_of[5], 71), 0),
        "master": bell_draw(streams_of[1], (2, DIN, KVH * HEAD), DIN ** -0.5, 0.09375, ((1, 128), (2, 8)), jnp.float32),
        "moment": bell_draw(streams_of[2], (2, DIN, KVH * HEAD), 0.01, 0.06, ((1, 128), (2, 8)), jnp.float32),
        "v_heads": jnp.clip(jnp.exp(math.log(0.001) - 2.3025852 * jax.random.uniform(streams_of[3], (KVH,), jnp.float32) ** level_of(streams_of[3], (KVH,), ((0, 8),), -0.2, 0.2)), 0.0001, 0.001),
        "v_neurons": jnp.clip(jnp.exp(math.log(0.001) - 2.3025852 * jax.random.uniform(streams_of[4], (KVH * HEAD,), jnp.float32) ** level_of(streams_of[4], (KVH * HEAD,), ((0, 8),), -0.2, 0.2)), 0.0001, 0.001),
    }


def reference(grads, master, moment, v_heads, v_neurons):

    def add_replica(index, total):
        return total + lax.dynamic_index_in_dim(grads, index, 0, keepdims=False).astype(jnp.float32)
    summed = lax.fori_loop(0, N_DP, add_replica, jnp.zeros(grads.shape[1:], jnp.float32))
    gradient = summed / N_DP
    keys = gradient[0].reshape(DIN, KVH, HEAD)
    head_sq = lax.optimization_barrier(jnp.sum(keys * keys, axis=(0, 2)))
    neuron_sq = lax.optimization_barrier(jnp.sum(gradient[1] * gradient[1], axis=0))
    total = jnp.sum(head_sq) + jnp.sum(neuron_sq)
    clip = jnp.minimum(1.0, 256.0 / (jnp.sqrt(total) + 1e-06))
    new_moment = 0.9 * moment + 0.1 * clip * gradient
    new_heads = 0.95 * v_heads + 0.05 * clip * clip * head_sq / (DIN * HEAD)
    new_neurons = 0.95 * v_neurons + 0.05 * clip * clip * neuron_sq / DIN
    second_fix = 1.0 - 0.95 ** STEP
    first_fix = 1.0 - 0.9 ** STEP
    key_denom = jnp.repeat(jnp.sqrt(new_heads / second_fix) + 1e-08, HEAD)
    value_denom = jnp.sqrt(new_neurons / second_fix) + 1e-08
    denom = jnp.stack([key_denom, value_denom])
    update = new_moment / first_fix / denom[:, None, :]
    new_master = master - 0.01 * (update + 0.1 * master)
    params = new_master.astype(jnp.bfloat16)
    return (params, new_master, new_moment, new_heads, new_neurons)
```

```python
import functools

import jax
import jax.numpy as jnp
from jax import lax
from jax.experimental import pallas as pl
from jax.experimental.pallas import tpu as pltpu
from jax.sharding import Mesh
from jax.sharding import PartitionSpec as P

DIN = 4096
HEAD = 128
STEP = 2
DP = ("z", "y", "c")
NZ, NY, NC, NX = 8, 8, 2, 8
ROWS = 32
SECOND_FIX = 1.0 - 0.95**STEP
FIRST_FIX = 1.0 - 0.9**STEP


def flat(z, y, c):
    return (z * NY + y) * NC + c


ALONG_Z = [[flat(z, y, c) for z in range(NZ)] for y in range(NY) for c in range(NC)]
Z_THEN_Y = [[flat(z, y, 0) for z in range(NZ)] for y in range(NY)] + [
    [flat(z, y, 1) for y in range(NY)] for z in range(NZ)
]
Y_THEN_Z = [[flat(z, y, 0) for y in range(NY)] for z in range(NZ)] + [
    [flat(z, y, 1) for z in range(NZ)] for y in range(NY)
]


def exchange(blocks, axes, groups=None):
    return lax.all_to_all(blocks, axes, split_axis=0, concat_axis=0, tiled=True, axis_index_groups=groups)


def swap_cores(x):
    return lax.ppermute(x, "c", [(0, 1), (1, 0)])


def pair_sum_kernel(core_ref, mine_ref, got_ref, out_ref, power_ref):
    core = core_ref[0]

    def add(i, top):
        hi, lo = i // 8, i % 8
        source = jnp.where(core == 0, i, lo * 8 + hi)
        for p in range(2):
            total = mine_ref[p, source].astype(jnp.float32) + got_ref[p, source].astype(jnp.float32)
            out_ref[i, p] = total
            top = jnp.maximum(top, jnp.max(jnp.abs(total).reshape(4, 8, 128), axis=0))
        return top

    top = lax.fori_loop(0, 64, add, jnp.zeros((8, 128), jnp.float32), unroll=4)
    largest = jnp.max(jnp.max(top, axis=0, keepdims=True), axis=1, keepdims=True)
    power = jnp.floor(jnp.log2(jnp.maximum(jnp.broadcast_to(largest, (8, 128)), 2.0**-100)))
    power_ref[...] = power
    scale = jnp.exp2(14.0 - power)[:1]

    def rescale(i, carry):
        for p in range(2):
            out_ref[i, p] = out_ref[i, p] * scale
        return carry

    lax.fori_loop(0, 64, rescale, 0, unroll=4)


def pair_sum(core, mine, got):
    vmem = pl.BlockSpec(memory_space=pltpu.VMEM)
    return pl.pallas_call(
        pair_sum_kernel,
        in_specs=[pl.BlockSpec(memory_space=pltpu.SMEM), vmem, vmem],
        out_specs=[vmem, vmem],
        out_shape=[
            jax.ShapeDtypeStruct((64, 2, ROWS, HEAD), jnp.float32),
            jax.ShapeDtypeStruct((8, HEAD), jnp.float32),
        ],
        name="pair_sum",
    )(core, mine, got)


def gradient_kernel(parts_ref, gradient_ref, send_ref):
    total = parts_ref[0]
    for k in range(1, 8):
        total = total + parts_ref[k]
    gradient = total / 128.0
    gradient_ref[...] = gradient
    squares = gradient * gradient
    head = jnp.sum(jnp.sum(squares[0], axis=0, keepdims=True), axis=1, keepdims=True)
    send_ref[:, 0:1, :] = jnp.broadcast_to(jnp.sum(squares[1], axis=0, keepdims=True)[None], (16, 1, HEAD))
    send_ref[:, 1:2, :] = jnp.broadcast_to(head[None], (16, 1, HEAD))


def gradient_of(parts):
    vmem = pl.BlockSpec(memory_space=pltpu.VMEM)
    return pl.pallas_call(
        gradient_kernel,
        in_specs=[vmem],
        out_specs=[vmem, vmem],
        out_shape=[
            jax.ShapeDtypeStruct((2, ROWS, HEAD), jnp.float32),
            jax.ShapeDtypeStruct((16, 2, HEAD), jnp.float32),
        ],
        name="gradient",
    )(parts)


def chip_stats_kernel(x_ref, got_ref, send_ref):
    x = x_ref[0]
    everyone = jnp.sum(got_ref[...], axis=0)
    lane = lax.broadcasted_iota(jnp.int32, (1, HEAD), 1)
    total = jnp.sum(everyone[0:1], axis=1, keepdims=True) + everyone[1:2]
    mine = got_ref[x] + got_ref[x + NX]
    send_ref[:, 0:1, :] = jnp.broadcast_to(mine[0:1][None], (64, 1, HEAD))
    send_ref[:, 1:2, :] = jnp.broadcast_to(jnp.where(lane == 0, mine[1:2], total)[None], (64, 1, HEAD))


def chip_stats(x, got):
    vmem = pl.BlockSpec(memory_space=pltpu.VMEM)
    return pl.pallas_call(
        chip_stats_kernel,
        in_specs=[pl.BlockSpec(memory_space=pltpu.SMEM), vmem],
        out_specs=vmem,
        out_shape=jax.ShapeDtypeStruct((64, 2, HEAD), jnp.float32),
        name="chip_stats",
    )(x, got)


def update_kernel(stats_ref, gradient_ref, master_ref, moment_ref, heads_ref, neurons_ref,
                  send_ref, new_master_ref, new_moment_ref, new_heads_ref, new_neurons_ref):
    stats = jnp.sum(stats_ref[...], axis=0)
    neuron_sq, other = stats[0:1], stats[1:2]
    lane = lax.broadcasted_iota(jnp.int32, (1, HEAD), 1)
    head_sq = jnp.sum(jnp.where(lane == 0, other, 0.0), axis=1, keepdims=True)
    total = jnp.sum(jnp.where(lane == 1, other, 0.0), axis=1, keepdims=True)
    clip = jnp.minimum(1.0, 256.0 / (jnp.sqrt(jnp.broadcast_to(total, (1, HEAD))) + 1e-06))
    new_heads = 0.95 * heads_ref[...] + 0.05 * clip * clip * head_sq / (DIN * HEAD)
    new_neurons = 0.95 * neurons_ref[...] + 0.05 * clip * clip * neuron_sq / DIN
    new_heads_ref[...] = new_heads
    new_neurons_ref[...] = new_neurons
    for p, second in ((0, new_heads), (1, new_neurons)):
        denom = jnp.sqrt(second / SECOND_FIX) + 1e-08
        new_moment = 0.9 * moment_ref[p] + 0.1 * clip * gradient_ref[p]
        update = new_moment / FIRST_FIX / denom
        master = master_ref[p]
        new_master = master - 0.01 * (update + 0.1 * master)
        new_moment_ref[p] = new_moment
        new_master_ref[p] = new_master
        params = new_master.astype(jnp.bfloat16)
        for k in range(8):
            send_ref[k, p] = params


def update_of(stats, gradient, master, moment, heads, neurons):
    vmem = pl.BlockSpec(memory_space=pltpu.VMEM)
    own = jax.ShapeDtypeStruct((2, ROWS, HEAD), jnp.float32)
    row = jax.ShapeDtypeStruct((1, HEAD), jnp.float32)
    return pl.pallas_call(
        update_kernel,
        in_specs=[vmem] * 6,
        out_specs=[vmem] * 5,
        out_shape=[jax.ShapeDtypeStruct((8, 2, ROWS, HEAD), jnp.bfloat16), own, own, row, row],
        name="update",
    )(stats, gradient, master, moment, heads, neurons)


def assemble_kernel(core_ref, mine_ref, got_ref, out_ref):
    core = core_ref[0]

    def place(i, carry):
        hi, lo = i // 8, i % 8
        turned = lo * 8 + hi
        for p in range(2):
            out_ref[p, jnp.where(core == 0, i, turned), core] = mine_ref[i, p]
            out_ref[p, jnp.where(core == 0, turned, i), 1 - core] = got_ref[i, p]
        return carry

    lax.fori_loop(0, 64, place, 0, unroll=4)


def assemble(core, mine, got):
    vmem = pl.BlockSpec(memory_space=pltpu.VMEM)
    return pl.pallas_call(
        assemble_kernel,
        in_specs=[pl.BlockSpec(memory_space=pltpu.SMEM), vmem, vmem],
        out_specs=vmem,
        out_shape=jax.ShapeDtypeStruct((2, 64, 2, ROWS, HEAD), jnp.bfloat16),
        name="assemble",
    )(core, mine, got)


def on_device(grads, master, moment, v_heads, v_neurons):
    c = lax.axis_index("c")
    core = c.reshape(1).astype(jnp.int32)
    x = lax.axis_index("x").reshape(1).astype(jnp.int32)

    halves = grads[0].reshape(2, 64, 2, ROWS, HEAD)
    theirs = lax.dynamic_index_in_dim(halves, 1 - c, 2, keepdims=False)
    mine = lax.dynamic_index_in_dim(halves, c, 2, keepdims=False)
    sums, power = pair_sum(core, mine, swap_cores(theirs))

    message = jnp.concatenate(
        [
            sums.reshape(8, 512, HEAD).astype(jnp.float16),
            jnp.broadcast_to(power.astype(jnp.float16), (8, 8, HEAD)),
        ],
        axis=1,
    )
    got = exchange(message, DP, Z_THEN_Y)
    scale = jnp.exp2(got[:, 512, 0].astype(jnp.float32) - 14.0)
    partial = jnp.sum(got[:, :512].astype(jnp.float32) * scale[:, None, None], axis=0)
    parts = exchange(partial.reshape(8, 2 * ROWS, HEAD), DP, Y_THEN_Z)

    gradient, send = gradient_of(parts.reshape(8, 2, ROWS, HEAD))
    send = chip_stats(x, exchange(send, ("c", "x")))
    stats = exchange(send, DP, [[flat(z, y, k) for z in range(NZ) for y in range(NY)] for k in range(NC)])

    heads = jnp.broadcast_to(v_heads, (1, HEAD))
    copies, new_master, new_moment, new_heads, new_neurons = update_of(
        stats, gradient, master, moment, heads, v_neurons.reshape(1, HEAD)
    )
    line = exchange(copies.reshape(8, 2 * ROWS, HEAD), DP, Y_THEN_Z)
    plane = exchange(jnp.broadcast_to(line.reshape(1, 512, HEAD), (8, 512, HEAD)), DP, Z_THEN_Y)
    plane = plane.reshape(64, 2, ROWS, HEAD)
    params = assemble(core, plane, swap_cores(plane)).reshape(2, DIN, HEAD)
    return (params, new_master, new_moment, new_heads[0, :1], new_neurons.reshape(HEAD))


def solution(mesh):
    split = Mesh(mesh.devices.reshape(NZ, NY, NC, NX), ("z", "y", "c", "x"))
    return jax.shard_map(
        on_device,
        mesh=split,
        in_specs=(
            P(DP, None, None, "x"),
            P(None, DP, "x"),
            P(None, DP, "x"),
            P("x"),
            P("x"),
        ),
        out_specs=(
            P(None, None, "x"),
            P(None, DP, "x"),
            P(None, DP, "x"),
            P("x"),
            P("x"),
        ),
        check_vma=False,
    )
```

```python
import jax
import jax.numpy as jnp
from jax import lax
from jax.experimental import pallas as pl
from jax.experimental.pallas import tpu as pltpu
from jax.sharding import Mesh
from jax.sharding import PartitionSpec as P

DIN = 4096
HEAD = 128
STEP = 2
DP = ("z", "y", "c")
NZ, NY, NC, NX = 8, 8, 2, 8
ROWS = 32
SECOND_FIX = 1.0 - 0.95**STEP
FIRST_FIX = 1.0 - 0.9**STEP
LOW = 2048.0
SMALL_VMEM = pltpu.CompilerParams(vmem_limit_bytes=12 * 1024 * 1024)
VMEM = pl.BlockSpec(memory_space=pltpu.VMEM)
SMEM = pl.BlockSpec(memory_space=pltpu.SMEM)


def flat(z, y, c):
    return (z * NY + y) * NC + c


FIRST = [[flat(z, y, 0) for z in range(NZ)] for y in range(NY)] + [
    [flat(z, y, 1) for y in range(NY)] for z in range(NZ)
]
SECOND = [[flat(z, y, 0) for y in range(NY)] for z in range(NZ)] + [
    [flat(z, y, 1) for z in range(NZ)] for y in range(NY)
]
STATS = [[device * NX + x for device in line for x in range(NX)] for line in FIRST]


def exchange(blocks, axes, groups):
    return lax.all_to_all(blocks, axes, split_axis=0, concat_axis=0, tiled=True, axis_index_groups=groups)


def swap_cores(x):
    return lax.ppermute(x, "c", [(0, 1), (1, 0)])


def power_of(values):
    return jnp.floor(jnp.log2(jnp.maximum(jnp.max(jnp.abs(values)), 2.0**-100)))


def as_half(values, power):
    return (values * jnp.exp2(14.0 - power)).astype(jnp.float16)


def in_two(values, power):
    scaled = values * jnp.exp2(14.0 - power)
    high = lax.reduce_precision(scaled, 5, 10)
    low = (scaled - high) * LOW
    return [high.astype(jnp.float16).reshape(2 * ROWS, HEAD), low.astype(jnp.float16).reshape(2 * ROWS, HEAD)]


def rows_of(*powers):
    lane = lax.broadcasted_iota(jnp.int32, (8, HEAD), 1)
    row = jnp.zeros((8, HEAD), jnp.float32)
    for k, power in enumerate(powers):
        row = jnp.where(lane == k, power, row)
    return row.astype(jnp.float16)


def out_of_two(high, low, scale):
    return (high.astype(jnp.float32) + low.astype(jnp.float32) * (1.0 / LOW)) * scale[:, None, None]


def scale_at(got, row, lane):
    return jnp.exp2(got[:, row, lane].astype(jnp.float32) - 14.0)


def core_stats_kernel(x_ref, got_ref, out_ref):
    everyone = jnp.sum(jnp.sum(got_ref[...], axis=0), axis=0)
    mine = jnp.sum(got_ref[:, x_ref[0]], axis=0)
    total = jnp.sum(everyone[0:1], axis=1, keepdims=True) + everyone[1:2]
    lane = lax.broadcasted_iota(jnp.int32, (1, HEAD), 1)
    out_ref[0:1] = mine[0:1]
    out_ref[1:2] = jnp.where(lane == 0, mine[1:2], total)


def core_stats(where, got):
    return pl.pallas_call(
        core_stats_kernel,
        in_specs=[SMEM, VMEM],
        out_specs=VMEM,
        out_shape=jax.ShapeDtypeStruct((2, HEAD), jnp.float32),
        compiler_params=SMALL_VMEM,
        name="core_stats",
    )(where, got)


def update_kernel(where_ref, stats_ref, other_ref, gradient_ref, master_ref, moment_ref, own_master_ref, own_moment_ref,
                  heads_ref, neurons_ref, params_ref, new_master_ref, new_moment_ref, new_heads_ref, new_neurons_ref):
    own = where_ref[1]
    stats = stats_ref[...] + other_ref[...]
    neuron_sq, other = stats[0:1], stats[1:2]
    lane = lax.broadcasted_iota(jnp.int32, (1, HEAD), 1)
    head_sq = jnp.broadcast_to(jnp.sum(jnp.where(lane == 0, other, 0.0), axis=1, keepdims=True), (1, HEAD))
    total = jnp.broadcast_to(jnp.sum(jnp.where(lane == 1, other, 0.0), axis=1, keepdims=True), (1, HEAD))
    clip = jnp.minimum(1.0, 256.0 / (jnp.sqrt(total) + 1e-06))
    new_heads = 0.95 * heads_ref[...] + 0.05 * clip * clip * head_sq / (DIN * HEAD)
    new_neurons = 0.95 * neurons_ref[...] + 0.05 * clip * clip * neuron_sq / DIN
    new_heads_ref[...] = new_heads
    new_neurons_ref[...] = new_neurons
    for p, second in ((0, new_heads), (1, new_neurons)):
        denom = jnp.sqrt(second / SECOND_FIX) + 1e-08

        def step(master, moment, gradient):
            new_moment = 0.9 * moment + 0.1 * clip * gradient
            update = new_moment / FIRST_FIX / denom
            return new_moment, master - 0.01 * (update + 0.1 * master)

        new_moment_ref[p], new_master_ref[p] = step(own_master_ref[p], own_moment_ref[p], gradient_ref[own, p])
        for k in range(8):
            _, new_master = step(master_ref[k, p], moment_ref[k, p], gradient_ref[k, p])
            params_ref[k, p] = new_master.astype(jnp.bfloat16)


def update_of(where, stats, other, gradient, master, moment, own_master, own_moment, heads, neurons):
    own = jax.ShapeDtypeStruct((2, ROWS, HEAD), jnp.float32)
    row = jax.ShapeDtypeStruct((1, HEAD), jnp.float32)
    return pl.pallas_call(
        update_kernel,
        in_specs=[SMEM] + [VMEM] * 9,
        out_specs=[VMEM] * 5,
        out_shape=[jax.ShapeDtypeStruct((8, 2, ROWS, HEAD), jnp.bfloat16), own, own, row, row],
        compiler_params=SMALL_VMEM,
        name="update",
    )(where, stats, other, gradient, master, moment, own_master, own_moment, heads, neurons)


def assemble_kernel(core_ref, mine_ref, got_ref, out_ref):
    core = core_ref[0]

    def place(i, carry):
        turned = (i % 8) * 8 + i // 8
        for p in range(2):
            out_ref[p, jnp.where(core == 0, i, turned), core] = mine_ref[i, p]
            out_ref[p, jnp.where(core == 0, turned, i), 1 - core] = got_ref[i, p]
        return carry

    lax.fori_loop(0, 64, place, 0, unroll=4)


def assemble(core, mine, got):
    return pl.pallas_call(
        assemble_kernel,
        in_specs=[SMEM, VMEM, VMEM],
        out_specs=VMEM,
        out_shape=jax.ShapeDtypeStruct((2, 64, 2, ROWS, HEAD), jnp.bfloat16),
        compiler_params=SMALL_VMEM,
        name="assemble",
    )(core, mine, got)


def on_device(grads, master, moment, v_heads, v_neurons):
    c = lax.axis_index("c")
    x = lax.axis_index("x")
    own = jnp.where(c == 0, lax.axis_index("y"), lax.axis_index("z"))

    where = jnp.stack([x, own]).astype(jnp.int32)
    core = c.reshape(1).astype(jnp.int32)
    halves = grads[0].reshape(2, 64, 2, ROWS, HEAD)
    theirs = lax.dynamic_index_in_dim(halves, 1 - c, 2, keepdims=False)
    halves, theirs = lax.optimization_barrier((halves, theirs))
    mine = lax.dynamic_index_in_dim(halves, c, 2, keepdims=False)
    power_a, power_o = power_of(master), power_of(moment)
    state = jnp.concatenate(in_two(master, power_a) + in_two(moment, power_o), axis=0)
    heads = jnp.broadcast_to(v_heads, (1, HEAD))
    neurons = v_neurons.reshape(1, HEAD)
    sums = mine.astype(jnp.float32) + swap_cores(theirs).astype(jnp.float32)
    power = power_of(sums)
    sums = sums.reshape(2, 8, 8, ROWS, HEAD)
    ordered = jnp.where(c == 0, sums.transpose(1, 2, 0, 3, 4), sums.transpose(2, 1, 0, 3, 4))
    message = jnp.concatenate(
        [as_half(ordered, power).reshape(8, 512, HEAD), jnp.broadcast_to(rows_of(power), (8, 8, HEAD))], axis=1
    )
    got = exchange(message, DP, FIRST)
    partial = jnp.sum(got[:, :512].astype(jnp.float32) * scale_at(got, 512, 0)[:, None, None], axis=0)

    power = power_of(partial)
    message = jnp.concatenate([as_half(partial, power), state, rows_of(power, power_a, power_o)], axis=0)
    message, where, core, heads = lax.optimization_barrier((message, where, core, heads))
    got = exchange(jnp.broadcast_to(message, (8, *message.shape)), DP, SECOND)
    gradient = jnp.sum(got[:, :512].astype(jnp.float32) * scale_at(got, 768, 0)[:, None, None], axis=0) / 128.0
    gradient = gradient.reshape(8, 2, ROWS, HEAD)
    squares = jnp.sum(gradient * gradient, axis=(0, 2))
    stats = jnp.stack([squares[1], jnp.broadcast_to(jnp.sum(squares[0]), (HEAD,))])
    stats = exchange(jnp.broadcast_to(stats, (64, 2, HEAD)), (*DP, "x"), STATS)
    stats = core_stats(where, stats.reshape(8, NX, 2, HEAD))

    line_master = out_of_two(got[:, 512:576], got[:, 576:640], scale_at(got, 768, 1)).reshape(8, 2, ROWS, HEAD)
    line_moment = out_of_two(got[:, 640:704], got[:, 704:768], scale_at(got, 768, 2)).reshape(8, 2, ROWS, HEAD)
    params, new_master, new_moment, new_heads, new_neurons = update_of(
        where, stats, swap_cores(stats), gradient, line_master, line_moment, master, moment, heads, neurons
    )
    plane = exchange(jnp.broadcast_to(params.reshape(512, HEAD), (8, 512, HEAD)), DP, FIRST)
    plane = plane.reshape(64, 2, ROWS, HEAD)
    params = assemble(core, plane, swap_cores(plane)).reshape(2, DIN, HEAD)
    return (params, new_master, new_moment, new_heads[0, :1], new_neurons.reshape(HEAD))


def solution(mesh):
    split = Mesh(mesh.devices.reshape(NZ, NY, NC, NX), ("z", "y", "c", "x"))
    return jax.shard_map(
        on_device,
        mesh=split,
        in_specs=(
            P(DP, None, None, "x"),
            P(None, DP, "x"),
            P(None, DP, "x"),
            P("x"),
            P("x"),
        ),
        out_specs=(
            P(None, None, "x"),
            P(None, DP, "x"),
            P(None, DP, "x"),
            P("x"),
            P("x"),
        ),
        check_vma=False,
    )
```

```python
import jax
import jax.numpy as jnp
from jax import lax
from jax.experimental import pallas as pl
from jax.experimental.pallas import tpu as pltpu
from jax.sharding import Mesh
from jax.sharding import PartitionSpec as P

DIN = 4096
HEAD = 128
STEP = 2
DP = ("z", "y", "c")
NZ, NY, NC, NX = 8, 8, 2, 8
ROWS = 32
SECOND_FIX = 1.0 - 0.95**STEP
FIRST_FIX = 1.0 - 0.9**STEP
SMALL_VMEM = pltpu.CompilerParams(vmem_limit_bytes=12 * 1024 * 1024)
VMEM = pl.BlockSpec(memory_space=pltpu.VMEM)
SMEM = pl.BlockSpec(memory_space=pltpu.SMEM)


def flat(z, y, c):
    return (z * NY + y) * NC + c


FIRST = [[flat(z, y, 0) for z in range(NZ)] for y in range(NY)] + [
    [flat(z, y, 1) for y in range(NY)] for z in range(NZ)
]
SECOND = [[flat(z, y, 0) for y in range(NY)] for z in range(NZ)] + [
    [flat(z, y, 1) for z in range(NZ)] for y in range(NY)
]
STATS = [[device * NX + x for device in line for x in range(NX)] for line in FIRST]


def exchange(blocks, axes, groups):
    return lax.all_to_all(blocks, axes, split_axis=0, concat_axis=0, tiled=True, axis_index_groups=groups)


def swap_cores(x):
    return lax.ppermute(x, "c", [(0, 1), (1, 0)])


def power_of(values):
    return jnp.floor(jnp.log2(jnp.maximum(jnp.max(jnp.abs(values)), 2.0**-100)))


def as_half(values, power):
    return (values * jnp.exp2(14.0 - power)).astype(jnp.float16)


def row_of(power):
    return jnp.full((8, HEAD), power, jnp.float16)


def scale_at(got):
    return jnp.exp2(got[:, 512, 0].astype(jnp.float32) - 14.0)


def summed(got):
    return jnp.sum(got[:, :512].astype(jnp.float32) * scale_at(got)[:, None, None], axis=0)


def line_stats_kernel(gradient_ref, out_ref):
    squares = [jnp.zeros((1, HEAD), jnp.float32)] * 2
    for p in range(2):
        for k in range(8):
            gradient = gradient_ref[k, p]
            squares[p] = squares[p] + jnp.sum(gradient * gradient, axis=0, keepdims=True)
    head = jnp.broadcast_to(jnp.sum(squares[0], axis=1, keepdims=True), (1, HEAD))
    out_ref[:, 0:1] = jnp.broadcast_to(squares[1][None], (64, 1, HEAD))
    out_ref[:, 1:2] = jnp.broadcast_to(head[None], (64, 1, HEAD))


def line_stats(gradient):
    return pl.pallas_call(
        line_stats_kernel,
        in_specs=[VMEM],
        out_specs=VMEM,
        out_shape=jax.ShapeDtypeStruct((64, 2, HEAD), jnp.float32),
        compiler_params=SMALL_VMEM,
        name="line_stats",
    )(gradient)


def core_stats_kernel(x_ref, got_ref, out_ref):
    everyone = jnp.sum(jnp.sum(got_ref[...], axis=0), axis=0)
    mine = jnp.sum(got_ref[:, x_ref[0]], axis=0)
    total = jnp.sum(everyone[0:1], axis=1, keepdims=True) + everyone[1:2]
    lane = lax.broadcasted_iota(jnp.int32, (1, HEAD), 1)
    out_ref[0:1] = mine[0:1]
    out_ref[1:2] = jnp.where(lane == 0, mine[1:2], total)


def core_stats(where, got):
    return pl.pallas_call(
        core_stats_kernel,
        in_specs=[SMEM, VMEM],
        out_specs=VMEM,
        out_shape=jax.ShapeDtypeStruct((2, HEAD), jnp.float32),
        compiler_params=SMALL_VMEM,
        name="core_stats",
    )(where, got)


def update_kernel(where_ref, stats_ref, other_ref, gradient_ref, state_ref,
                  heads_ref, neurons_ref, params_ref, new_master_ref, new_moment_ref, new_heads_ref, new_neurons_ref):
    own = where_ref[1]
    stats = stats_ref[...] + other_ref[...]
    neuron_sq, other = stats[0:1], stats[1:2]
    lane = lax.broadcasted_iota(jnp.int32, (1, HEAD), 1)
    head_sq = jnp.broadcast_to(jnp.sum(jnp.where(lane == 0, other, 0.0), axis=1, keepdims=True), (1, HEAD))
    total = jnp.broadcast_to(jnp.sum(jnp.where(lane == 1, other, 0.0), axis=1, keepdims=True), (1, HEAD))
    clip = jnp.minimum(1.0, 256.0 / (jnp.sqrt(total) + 1e-06))
    new_heads = 0.95 * heads_ref[...] + 0.05 * clip * clip * head_sq / (DIN * HEAD)
    new_neurons = 0.95 * neurons_ref[...] + 0.05 * clip * clip * neuron_sq / DIN
    new_heads_ref[...] = new_heads
    new_neurons_ref[...] = new_neurons
    for p, second in ((0, new_heads), (1, new_neurons)):
        denom = jnp.sqrt(second / SECOND_FIX) + 1e-08

        def step(master, moment, gradient):
            new_moment = 0.9 * moment + 0.1 * clip * gradient
            update = new_moment / FIRST_FIX / denom
            return new_moment, master - 0.01 * (update + 0.1 * master)

        new_moment_ref[p], new_master_ref[p] = step(state_ref[own, 0, p], state_ref[own, 1, p], gradient_ref[own, p])
        for k in range(8):
            _, new_master = step(state_ref[k, 0, p], state_ref[k, 1, p], gradient_ref[k, p])
            params_ref[k, p] = new_master.astype(jnp.bfloat16)


def update_of(where, stats, other, gradient, state, heads, neurons):
    own = jax.ShapeDtypeStruct((2, ROWS, HEAD), jnp.float32)
    row = jax.ShapeDtypeStruct((1, HEAD), jnp.float32)
    return pl.pallas_call(
        update_kernel,
        in_specs=[SMEM] + [VMEM] * 6,
        out_specs=[VMEM] * 5,
        out_shape=[jax.ShapeDtypeStruct((8, 2, ROWS, HEAD), jnp.bfloat16), own, own, row, row],
        compiler_params=SMALL_VMEM,
        name="update",
    )(where, stats, other, gradient, state, heads, neurons)


def assemble_kernel(core_ref, mine_ref, got_ref, out_ref):
    core = core_ref[0]

    def place(i, carry):
        turned = (i % 8) * 8 + i // 8
        for p in range(2):
            out_ref[p, jnp.where(core == 0, i, turned), core] = mine_ref[i, p]
            out_ref[p, jnp.where(core == 0, turned, i), 1 - core] = got_ref[i, p]
        return carry

    lax.fori_loop(0, 64, place, 0, unroll=4)


def assemble(core, mine, got):
    return pl.pallas_call(
        assemble_kernel,
        in_specs=[SMEM, VMEM, VMEM],
        out_specs=VMEM,
        out_shape=jax.ShapeDtypeStruct((2, 64, 2, ROWS, HEAD), jnp.bfloat16),
        compiler_params=SMALL_VMEM,
        name="assemble",
    )(core, mine, got)


def on_device(grads, master, moment, v_heads, v_neurons):
    c = lax.axis_index("c")
    x = lax.axis_index("x")
    own = jnp.where(c == 0, lax.axis_index("y"), lax.axis_index("z"))

    where = jnp.stack([x, own]).astype(jnp.int32)
    core = c.reshape(1).astype(jnp.int32)
    state = jnp.broadcast_to(jnp.stack([master, moment]).reshape(4 * ROWS, HEAD), (8, 4 * ROWS, HEAD))
    state = exchange(state, DP, SECOND)
    halves = grads[0].reshape(2, 64, 2, ROWS, HEAD)
    theirs = lax.dynamic_index_in_dim(halves, 1 - c, 2, keepdims=False)
    halves, theirs = lax.optimization_barrier((halves, theirs))
    mine = lax.dynamic_index_in_dim(halves, c, 2, keepdims=False)
    heads = jnp.broadcast_to(v_heads, (1, HEAD))
    neurons = v_neurons.reshape(1, HEAD)
    sums = mine.astype(jnp.float32) + swap_cores(theirs).astype(jnp.float32)
    power = power_of(sums)
    sums = sums.reshape(2, 8, 8, ROWS, HEAD)
    ordered = jnp.where(c == 0, sums.transpose(1, 2, 0, 3, 4), sums.transpose(2, 1, 0, 3, 4))
    message = jnp.concatenate(
        [as_half(ordered, power).reshape(8, 512, HEAD), jnp.broadcast_to(row_of(power), (8, 8, HEAD))], axis=1
    )
    message, where, core, heads, state = lax.optimization_barrier((message, where, core, heads, state))
    partial = summed(exchange(message, DP, FIRST))

    power = power_of(partial)
    message = lax.optimization_barrier(jnp.concatenate([as_half(partial, power), row_of(power)], axis=0))
    got = exchange(jnp.broadcast_to(message, (8, *message.shape)), DP, SECOND)
    gradient = (summed(got) / 128.0).reshape(8, 2, ROWS, HEAD)

    stats = line_stats(gradient)
    stats = exchange(stats, (*DP, "x"), STATS)
    stats = core_stats(where, stats.reshape(8, NX, 2, HEAD))
    params, new_master, new_moment, new_heads, new_neurons = update_of(
        where, stats, swap_cores(stats), gradient, state.reshape(8, 2, 2, ROWS, HEAD), heads, neurons
    )
    plane = exchange(jnp.broadcast_to(params.reshape(512, HEAD), (8, 512, HEAD)), DP, FIRST)
    plane = plane.reshape(64, 2, ROWS, HEAD)
    params = assemble(core, plane, swap_cores(plane)).reshape(2, DIN, HEAD)
    return (params, new_master, new_moment, new_heads[0, :1], new_neurons.reshape(HEAD))


def solution(mesh):
    split = Mesh(mesh.devices.reshape(NZ, NY, NC, NX), ("z", "y", "c", "x"))
    return jax.shard_map(
        on_device,
        mesh=split,
        in_specs=(
            P(DP, None, None, "x"),
            P(None, DP, "x"),
            P(None, DP, "x"),
            P("x"),
            P("x"),
        ),
        out_specs=(
            P(None, None, "x"),
            P(None, DP, "x"),
            P(None, DP, "x"),
            P("x"),
            P("x"),
        ),
        check_vma=False,
    )
```

```python
import jax
import jax.numpy as jnp
from jax import lax
from jax.experimental import pallas as pl
from jax.experimental.pallas import tpu as pltpu
from jax.sharding import Mesh
from jax.sharding import PartitionSpec as P

DIN = 4096
HEAD = 128
STEP = 2
DP = ("z", "y", "c")
NZ, NY, NC, NX = 8, 8, 2, 8
ROWS = 32
SECOND_FIX = 1.0 - 0.95**STEP
FIRST_FIX = 1.0 - 0.9**STEP
LOW = 2048.0
SMALL_VMEM = pltpu.CompilerParams(vmem_limit_bytes=12 * 1024 * 1024)
VMEM = pl.BlockSpec(memory_space=pltpu.VMEM)
SMEM = pl.BlockSpec(memory_space=pltpu.SMEM)
HBM = pl.BlockSpec(memory_space=pltpu.HBM)


def flat(z, y, c):
    return (z * NY + y) * NC + c


FIRST = [[flat(z, y, 0) for z in range(NZ)] for y in range(NY)] + [
    [flat(z, y, 1) for y in range(NY)] for z in range(NZ)
]
SECOND = [[flat(z, y, 0) for y in range(NY)] for z in range(NZ)] + [
    [flat(z, y, 1) for z in range(NZ)] for y in range(NY)
]
STATS = [
    [flat(z, j, 0) * NX + x for z in range(NZ) for x in range(NX)]
    + [flat(j, y, 1) * NX + x for y in range(NY) for x in range(NX)]
    for j in range(8)
]


def exchange(blocks, axes, groups):
    return lax.all_to_all(blocks, axes, split_axis=0, concat_axis=0, tiled=True, axis_index_groups=groups)


def swap_cores(x):
    return lax.ppermute(x, "c", [(0, 1), (1, 0)])


def power_of(values):
    return jnp.floor(jnp.log2(jnp.maximum(jnp.max(jnp.abs(values)), 2.0**-100)))


def as_half(values, power):
    return (values * jnp.exp2(14.0 - power)).astype(jnp.float16)


def in_two(values, power):
    scaled = values * jnp.exp2(14.0 - power)
    high = lax.reduce_precision(scaled, 5, 10)
    low = (scaled - high) * LOW
    return [high.astype(jnp.float16).reshape(2 * ROWS, HEAD), low.astype(jnp.float16).reshape(2 * ROWS, HEAD)]


def lane_row(k, power):
    lane = lax.broadcasted_iota(jnp.int32, (8, HEAD), 1)
    return jnp.where(lane == k, power, 0.0)


def out_of_two(high, low, scale):
    return (high.astype(jnp.float32) + low.astype(jnp.float32) * (1.0 / LOW)) * scale[:, None, None]


def scale_at(got, row, lane):
    return jnp.exp2(got[:, row, lane].astype(jnp.float32) - 14.0)


def line_stats_kernel(gradient_ref, out_ref):
    squares = [jnp.zeros((1, HEAD), jnp.float32)] * 2
    for p in range(2):
        for k in range(8):
            gradient = gradient_ref[k, p]
            squares[p] = squares[p] + jnp.sum(gradient * gradient, axis=0, keepdims=True)
    head = jnp.broadcast_to(jnp.sum(squares[0], axis=1, keepdims=True), (1, HEAD))
    out_ref[:, 0:1] = jnp.broadcast_to(squares[1][None], (128, 1, HEAD))
    out_ref[:, 1:2] = jnp.broadcast_to(head[None], (128, 1, HEAD))


def line_stats(gradient):
    return pl.pallas_call(
        line_stats_kernel,
        in_specs=[VMEM],
        out_specs=VMEM,
        out_shape=jax.ShapeDtypeStruct((128, 2, HEAD), jnp.float32),
        compiler_params=SMALL_VMEM,
        name="line_stats",
    )(gradient)


def update_kernel(where_ref, stats_ref, gradient_ref, master_ref, moment_ref, own_master_ref, own_moment_ref,
                  heads_ref, neurons_ref, params_ref, new_master_ref, new_moment_ref, new_heads_ref, new_neurons_ref):
    x, own = where_ref[0], where_ref[1]
    column = jnp.sum(jnp.sum(stats_ref[...], axis=0), axis=0)
    total = jnp.sum(column[0:1], axis=1, keepdims=True) + column[1:2]
    mine = jnp.sum(stats_ref[:, x], axis=0)
    neuron_sq, head_sq = mine[0:1], mine[1:2]
    clip = jnp.minimum(1.0, 256.0 / (jnp.sqrt(total) + 1e-06))
    new_heads = 0.95 * heads_ref[...] + 0.05 * clip * clip * head_sq / (DIN * HEAD)
    new_neurons = 0.95 * neurons_ref[...] + 0.05 * clip * clip * neuron_sq / DIN
    new_heads_ref[...] = new_heads
    new_neurons_ref[...] = new_neurons
    for p, second in ((0, new_heads), (1, new_neurons)):
        denom = jnp.sqrt(second / SECOND_FIX) + 1e-08

        def step(master, moment, gradient):
            new_moment = 0.9 * moment + 0.1 * clip * gradient
            update = new_moment / FIRST_FIX / denom
            return new_moment, master - 0.01 * (update + 0.1 * master)

        new_moment_ref[p], new_master_ref[p] = step(own_master_ref[p], own_moment_ref[p], gradient_ref[own, p])
        for k in range(8):
            _, new_master = step(master_ref[k, p], moment_ref[k, p], gradient_ref[k, p])
            params_ref[k, p] = new_master.astype(jnp.bfloat16)


def update_of(where, stats, gradient, master, moment, own_master, own_moment, heads, neurons):
    own = jax.ShapeDtypeStruct((2, ROWS, HEAD), jnp.float32)
    row = jax.ShapeDtypeStruct((1, HEAD), jnp.float32)
    return pl.pallas_call(
        update_kernel,
        in_specs=[SMEM] + [VMEM] * 8,
        out_specs=[VMEM] * 5,
        out_shape=[jax.ShapeDtypeStruct((8, 2, ROWS, HEAD), jnp.bfloat16), own, own, row, row],
        compiler_params=SMALL_VMEM,
        name="update",
    )(where, stats, gradient, master, moment, own_master, own_moment, heads, neurons)


def place_kernel(slot_ref, plane_ref, *rest):
    out_ref, sems = rest[-2:]
    slot = slot_ref[0]

    def copies(k):
        for hi in range(8):
            for p in range(2):
                source = plane_ref.at[hi, :, p] if k == 0 else plane_ref.at[:, hi, p]
                yield pltpu.make_async_copy(source, out_ref.at[p, hi, :, k], sems.at[hi, p])

    for k in range(2):

        @pl.when(slot == k)
        def _():
            for copy in copies(k):
                copy.start()
            for copy in copies(k):
                copy.wait()


def place(slot, plane, before, name):
    before = () if before is None else (before,)
    return pl.pallas_call(
        place_kernel,
        in_specs=[SMEM, VMEM] + [HBM] * len(before),
        out_specs=HBM,
        out_shape=jax.ShapeDtypeStruct((2, 8, 8, 2, ROWS, HEAD), jnp.bfloat16),
        scratch_shapes=[pltpu.SemaphoreType.DMA((8, 2))],
        input_output_aliases={2: 0} if before else {},
        compiler_params=SMALL_VMEM,
        name=name,
    )(slot, plane, *before)


def on_device(grads, master, moment, v_heads, v_neurons):
    c = lax.axis_index("c")
    x = lax.axis_index("x")
    own = jnp.where(c == 0, lax.axis_index("y"), lax.axis_index("z"))

    where = jnp.stack([x, own]).astype(jnp.int32)
    core = c.reshape(1).astype(jnp.int32)
    halves = grads[0].reshape(2, 64, 2, ROWS, HEAD)
    theirs = lax.dynamic_index_in_dim(halves, 1 - c, 2, keepdims=False)
    halves, theirs = lax.optimization_barrier((halves, theirs))
    mine = lax.dynamic_index_in_dim(halves, c, 2, keepdims=False)
    power_a, power_o = power_of(master), power_of(moment)
    state = jnp.concatenate(in_two(master, power_a) + in_two(moment, power_o), axis=0)
    heads = jnp.broadcast_to(v_heads, (1, HEAD))
    neurons = v_neurons.reshape(1, HEAD)
    sums = mine.astype(jnp.float32) + swap_cores(theirs).astype(jnp.float32)
    power = power_of(sums)
    sums = sums.reshape(2, 8, 8, ROWS, HEAD)
    ordered = jnp.where(c == 0, sums.transpose(1, 2, 0, 3, 4), sums.transpose(2, 1, 0, 3, 4))
    message = jnp.concatenate(
        [as_half(ordered, power).reshape(8, 512, HEAD), jnp.broadcast_to(lane_row(0, power).astype(jnp.float16), (8, 8, HEAD))], axis=1
    )
    first_lane, powers = lane_row(0, 1.0), lane_row(1, power_a) + lane_row(2, power_o)
    message, state, first_lane, powers, where, core, heads = lax.optimization_barrier(
        (message, state, first_lane, powers, where, core, heads)
    )
    got = exchange(message, DP, FIRST)
    partial = jnp.sum(got[:, :512].astype(jnp.float32) * scale_at(got, 512, 0)[:, None, None], axis=0)

    power = power_of(partial)
    message = jnp.concatenate([as_half(partial, power), state, (powers + power * first_lane).astype(jnp.float16)], axis=0)
    message = lax.optimization_barrier(message)
    got = exchange(jnp.broadcast_to(message, (8, *message.shape)), DP, SECOND)
    gradient = jnp.sum(got[:, :512].astype(jnp.float32) * scale_at(got, 768, 0)[:, None, None], axis=0) / 128.0
    gradient = gradient.reshape(8, 2, ROWS, HEAD)
    stats = exchange(line_stats(gradient), (*DP, "x"), STATS)
    line_master = out_of_two(got[:, 512:576], got[:, 576:640], scale_at(got, 768, 1)).reshape(8, 2, ROWS, HEAD)
    line_moment = out_of_two(got[:, 640:704], got[:, 704:768], scale_at(got, 768, 2)).reshape(8, 2, ROWS, HEAD)
    params, new_master, new_moment, new_heads, new_neurons = update_of(
        where, stats.reshape(16, NX, 2, HEAD), gradient, line_master, line_moment, master, moment, heads, neurons
    )
    plane = exchange(jnp.broadcast_to(params.reshape(512, HEAD), (8, 512, HEAD)), DP, FIRST)
    plane = plane.reshape(8, 8, 2, ROWS, HEAD)
    other = swap_cores(plane)
    params = place(core, plane, None, "place_mine")
    params = place(1 - core, other, params, "place_theirs").reshape(2, DIN, HEAD)
    return (params, new_master, new_moment, new_heads[0, :1], new_neurons.reshape(HEAD))


def solution(mesh):
    split = Mesh(mesh.devices.reshape(NZ, NY, NC, NX), ("z", "y", "c", "x"))
    return jax.shard_map(
        on_device,
        mesh=split,
        in_specs=(
            P(DP, None, None, "x"),
            P(None, DP, "x"),
            P(None, DP, "x"),
            P("x"),
            P("x"),
        ),
        out_specs=(
            P(None, None, "x"),
            P(None, DP, "x"),
            P(None, DP, "x"),
            P("x"),
            P("x"),
        ),
        check_vma=False,
    )
```

```python
import jax
import jax.numpy as jnp
from jax import lax
from jax.experimental import pallas as pl
from jax.experimental.pallas import tpu as pltpu
from jax.sharding import Mesh
from jax.sharding import PartitionSpec as P

DIN = 4096
HEAD = 128
STEP = 2
DP = ("z", "y", "c")
NZ, NY, NC, NX = 8, 8, 2, 8
ROWS = 32
SECOND_FIX = 1.0 - 0.95**STEP
FIRST_FIX = 1.0 - 0.9**STEP
LOW = 2048.0
SMALL_VMEM = pltpu.CompilerParams(vmem_limit_bytes=12 * 1024 * 1024)
VMEM = pl.BlockSpec(memory_space=pltpu.VMEM)
SMEM = pl.BlockSpec(memory_space=pltpu.SMEM)
HBM = pl.BlockSpec(memory_space=pltpu.HBM)


def flat(z, y, c):
    return (z * NY + y) * NC + c


FIRST = [[flat(z, y, 0) for z in range(NZ)] for y in range(NY)] + [
    [flat(z, y, 1) for y in range(NY)] for z in range(NZ)
]
SECOND = [[flat(z, y, 0) for y in range(NY)] for z in range(NZ)] + [
    [flat(z, y, 1) for z in range(NZ)] for y in range(NY)
]
STATS = [
    [flat(z, j, 0) * NX + x for z in range(NZ) for x in range(NX)]
    + [flat(j, y, 1) * NX + x for y in range(NY) for x in range(NX)]
    for j in range(8)
]


def exchange(blocks, axes, groups):
    return lax.all_to_all(blocks, axes, split_axis=0, concat_axis=0, tiled=True, axis_index_groups=groups)


def swap_cores(x):
    return lax.ppermute(x, "c", [(0, 1), (1, 0)])


def power_of(values, axes):
    largest = jnp.max(jnp.abs(values), axis=axes)
    return jnp.floor(jnp.log2(jnp.maximum(largest, 2.0**-100)))


def as_half(values, power):
    return (values * jnp.exp2(14.0 - power)).astype(jnp.float16)


def in_two(values, power):
    scaled = values * jnp.exp2(14.0 - power)
    high = lax.reduce_precision(scaled, 5, 10)
    low = (scaled - high) * LOW
    return [high.astype(jnp.float16).reshape(2 * ROWS, HEAD), low.astype(jnp.float16).reshape(2 * ROWS, HEAD)]


def row_at(k, power):
    row = lax.broadcasted_iota(jnp.int32, (8, HEAD), 0)
    return jnp.where(row == k, power, 0.0)


def out_of_two(high, low, scale):
    return (high.astype(jnp.float32) + low.astype(jnp.float32) * (1.0 / LOW)) * scale[:, None, :]


def scale_at(got, row):
    return jnp.exp2(got[:, row].astype(jnp.float32) - 14.0)


def line_stats_kernel(gradient_ref, out_ref):
    squares = [jnp.zeros((1, HEAD), jnp.float32)] * 2
    for p in range(2):
        for k in range(8):
            gradient = gradient_ref[k, p]
            squares[p] = squares[p] + jnp.sum(gradient * gradient, axis=0, keepdims=True)
    head = jnp.broadcast_to(jnp.sum(squares[0], axis=1, keepdims=True), (1, HEAD))
    out_ref[:, 0:1] = jnp.broadcast_to(squares[1][None], (128, 1, HEAD))
    out_ref[:, 1:2] = jnp.broadcast_to(head[None], (128, 1, HEAD))


def line_stats(gradient):
    return pl.pallas_call(
        line_stats_kernel,
        in_specs=[VMEM],
        out_specs=VMEM,
        out_shape=jax.ShapeDtypeStruct((128, 2, HEAD), jnp.float32),
        compiler_params=SMALL_VMEM,
        name="line_stats",
    )(gradient)


def update_kernel(where_ref, stats_ref, gradient_ref, master_ref, moment_ref, own_master_ref, own_moment_ref,
                  heads_ref, neurons_ref, params_ref, new_master_ref, new_moment_ref, new_heads_ref, new_neurons_ref):
    x, own = where_ref[0], where_ref[1]
    column = jnp.sum(jnp.sum(stats_ref[...], axis=0), axis=0)
    total = jnp.sum(column[0:1], axis=1, keepdims=True) + column[1:2]
    mine = jnp.sum(stats_ref[:, x], axis=0)
    neuron_sq, head_sq = mine[0:1], mine[1:2]
    clip = jnp.minimum(1.0, 256.0 / (jnp.sqrt(total) + 1e-06))
    new_heads = 0.95 * heads_ref[...] + 0.05 * clip * clip * head_sq / (DIN * HEAD)
    new_neurons = 0.95 * neurons_ref[...] + 0.05 * clip * clip * neuron_sq / DIN
    new_heads_ref[...] = new_heads
    new_neurons_ref[...] = new_neurons
    for p, second in ((0, new_heads), (1, new_neurons)):
        denom = jnp.sqrt(second / SECOND_FIX) + 1e-08

        def step(master, moment, gradient):
            new_moment = 0.9 * moment + 0.1 * clip * gradient
            update = new_moment / FIRST_FIX / denom
            return new_moment, master - 0.01 * (update + 0.1 * master)

        new_moment_ref[p], new_master_ref[p] = step(own_master_ref[p], own_moment_ref[p], gradient_ref[own, p])
        for k in range(8):
            _, new_master = step(master_ref[k, p], moment_ref[k, p], gradient_ref[k, p])
            params_ref[k, p] = new_master.astype(jnp.bfloat16)


def update_of(where, stats, gradient, master, moment, own_master, own_moment, heads, neurons):
    own = jax.ShapeDtypeStruct((2, ROWS, HEAD), jnp.float32)
    row = jax.ShapeDtypeStruct((1, HEAD), jnp.float32)
    return pl.pallas_call(
        update_kernel,
        in_specs=[SMEM] + [VMEM] * 8,
        out_specs=[VMEM] * 5,
        out_shape=[jax.ShapeDtypeStruct((8, 2, ROWS, HEAD), jnp.bfloat16), own, own, row, row],
        compiler_params=SMALL_VMEM,
        name="update",
    )(where, stats, gradient, master, moment, own_master, own_moment, heads, neurons)


def place_kernel(slot_ref, plane_ref, *rest):
    out_ref, sems = rest[-2:]
    slot = slot_ref[0]

    def copies(k):
        for hi in range(8):
            for p in range(2):
                source = plane_ref.at[hi, :, p] if k == 0 else plane_ref.at[:, hi, p]
                yield pltpu.make_async_copy(source, out_ref.at[p, hi, :, k], sems.at[hi, p])

    for k in range(2):

        @pl.when(slot == k)
        def _():
            for copy in copies(k):
                copy.start()
            for copy in copies(k):
                copy.wait()


def place(slot, plane, before, name):
    before = () if before is None else (before,)
    return pl.pallas_call(
        place_kernel,
        in_specs=[SMEM, VMEM] + [HBM] * len(before),
        out_specs=HBM,
        out_shape=jax.ShapeDtypeStruct((2, 8, 8, 2, ROWS, HEAD), jnp.bfloat16),
        scratch_shapes=[pltpu.SemaphoreType.DMA((8, 2))],
        input_output_aliases={2: 0} if before else {},
        compiler_params=SMALL_VMEM,
        name=name,
    )(slot, plane, *before)


def on_device(grads, master, moment, v_heads, v_neurons):
    c = lax.axis_index("c")
    x = lax.axis_index("x")
    own = jnp.where(c == 0, lax.axis_index("y"), lax.axis_index("z"))

    where = jnp.stack([x, own]).astype(jnp.int32)
    core = c.reshape(1).astype(jnp.int32)
    halves = grads[0].reshape(2, 64, 2, ROWS, HEAD)
    theirs = lax.dynamic_index_in_dim(halves, 1 - c, 2, keepdims=False)
    halves, theirs = lax.optimization_barrier((halves, theirs))
    mine = lax.dynamic_index_in_dim(halves, c, 2, keepdims=False)
    power_a, power_o = power_of(master, (0, 1)), power_of(moment, (0, 1))
    state = jnp.concatenate(in_two(master, power_a) + in_two(moment, power_o), axis=0)
    heads = jnp.broadcast_to(v_heads, (1, HEAD))
    neurons = v_neurons.reshape(1, HEAD)
    sums = mine.astype(jnp.float32) + swap_cores(theirs).astype(jnp.float32)
    power = power_of(sums, None)
    sums = sums.reshape(2, 8, 8, ROWS, HEAD)
    ordered = jnp.where(c == 0, sums.transpose(1, 2, 0, 3, 4), sums.transpose(2, 1, 0, 3, 4))
    message = jnp.concatenate(
        [as_half(ordered, power).reshape(8, 512, HEAD), jnp.full((8, 8, HEAD), power, jnp.float16)], axis=1
    )
    first_row, powers = row_at(0, 1.0), row_at(1, power_a) + row_at(2, power_o)
    message, state, first_row, powers, where, core, heads = lax.optimization_barrier(
        (message, state, first_row, powers, where, core, heads)
    )
    got = exchange(message, DP, FIRST)
    partial = jnp.sum(got[:, :512].astype(jnp.float32) * scale_at(got, 512)[:, None, :], axis=0)

    power = power_of(partial, 0)
    message = jnp.concatenate([as_half(partial, power), state, (powers + power * first_row).astype(jnp.float16)], axis=0)
    message = lax.optimization_barrier(message)
    got = exchange(jnp.broadcast_to(message, (8, *message.shape)), DP, SECOND)
    gradient = jnp.sum(got[:, :512].astype(jnp.float32) * scale_at(got, 768)[:, None, :], axis=0) / 128.0
    gradient = gradient.reshape(8, 2, ROWS, HEAD)
    stats = exchange(line_stats(gradient), (*DP, "x"), STATS)
    line_master = out_of_two(got[:, 512:576], got[:, 576:640], scale_at(got, 769)).reshape(8, 2, ROWS, HEAD)
    line_moment = out_of_two(got[:, 640:704], got[:, 704:768], scale_at(got, 770)).reshape(8, 2, ROWS, HEAD)
    params, new_master, new_moment, new_heads, new_neurons = update_of(
        where, stats.reshape(16, NX, 2, HEAD), gradient, line_master, line_moment, master, moment, heads, neurons
    )
    plane = exchange(jnp.broadcast_to(params.reshape(512, HEAD), (8, 512, HEAD)), DP, FIRST)
    plane = plane.reshape(8, 8, 2, ROWS, HEAD)
    other = swap_cores(plane)
    params = place(core, plane, None, "place_mine")
    params = place(1 - core, other, params, "place_theirs").reshape(2, DIN, HEAD)
    return (params, new_master, new_moment, new_heads[0, :1], new_neurons.reshape(HEAD))


def solution(mesh):
    split = Mesh(mesh.devices.reshape(NZ, NY, NC, NX), ("z", "y", "c", "x"))
    return jax.shard_map(
        on_device,
        mesh=split,
        in_specs=(
            P(DP, None, None, "x"),
            P(None, DP, "x"),
            P(None, DP, "x"),
            P("x"),
            P("x"),
        ),
        out_specs=(
            P(None, None, "x"),
            P(None, DP, "x"),
            P(None, DP, "x"),
            P("x"),
            P("x"),
        ),
        check_vma=False,
    )
```

```python
import jax
import jax.numpy as jnp
from jax import lax
from jax.experimental import pallas as pl
from jax.experimental.pallas import tpu as pltpu
from jax.sharding import Mesh
from jax.sharding import PartitionSpec as P

DIN = 4096
HEAD = 128
STEP = 2
DP = ("z", "y", "c")
NZ, NY, NC, NX = 8, 8, 2, 8
ROWS = 32
SECOND_FIX = 1.0 - 0.95**STEP
FIRST_FIX = 1.0 - 0.9**STEP
LOW = 2048.0
SMALL_VMEM = pltpu.CompilerParams(vmem_limit_bytes=12 * 1024 * 1024)
VMEM = pl.BlockSpec(memory_space=pltpu.VMEM)
SMEM = pl.BlockSpec(memory_space=pltpu.SMEM)
HBM = pl.BlockSpec(memory_space=pltpu.HBM)


def flat(z, y, c):
    return (z * NY + y) * NC + c


FIRST = [[flat(z, y, 0) for z in range(NZ)] for y in range(NY)] + [
    [flat(z, y, 1) for y in range(NY)] for z in range(NZ)
]
SECOND = [[flat(z, y, 0) for y in range(NY)] for z in range(NZ)] + [
    [flat(z, y, 1) for z in range(NZ)] for y in range(NY)
]
STATS = [
    [flat(z, j, 0) * NX + x for z in range(NZ) for x in range(NX)]
    + [flat(j, y, 1) * NX + x for y in range(NY) for x in range(NX)]
    for j in range(8)
]


def exchange(blocks, axes, groups):
    return lax.all_to_all(blocks, axes, split_axis=0, concat_axis=0, tiled=True, axis_index_groups=groups)


def swap_cores(x):
    return lax.ppermute(x, "c", [(0, 1), (1, 0)])


def power_of(values, axes):
    largest = jnp.max(jnp.abs(values), axis=axes)
    return jnp.floor(jnp.log2(jnp.maximum(largest, 2.0**-100)))


def as_half(values, power):
    return (values * jnp.exp2(14.0 - power)).astype(jnp.float16)


def in_two(values, power):
    scaled = values * jnp.exp2(14.0 - power)
    high = lax.reduce_precision(scaled, 5, 10)
    low = (scaled - high) * LOW
    return [high.astype(jnp.float16).reshape(2 * ROWS, HEAD), low.astype(jnp.float16).reshape(2 * ROWS, HEAD)]


def row_at(k, power):
    row = lax.broadcasted_iota(jnp.int32, (8, HEAD), 0)
    return jnp.where(row == k, power, 0.0)


def out_of_two(high, low, scale):
    return (high.astype(jnp.float32) + low.astype(jnp.float32) * (1.0 / LOW)) * scale[:, None, :]


def scale_at(got, row):
    return jnp.exp2(got[:, row].astype(jnp.float32) - 14.0)


def line_stats_kernel(gradient_ref, out_ref):
    squares = [jnp.zeros((1, HEAD), jnp.float32)] * 2
    for p in range(2):
        for k in range(8):
            gradient = gradient_ref[k, p]
            squares[p] = squares[p] + jnp.sum(gradient * gradient, axis=0, keepdims=True)
    head = jnp.broadcast_to(jnp.sum(squares[0], axis=1, keepdims=True), (1, HEAD))
    out_ref[:, 0:1] = jnp.broadcast_to(squares[1][None], (128, 1, HEAD))
    out_ref[:, 1:2] = jnp.broadcast_to(head[None], (128, 1, HEAD))


def line_stats(gradient):
    return pl.pallas_call(
        line_stats_kernel,
        in_specs=[VMEM],
        out_specs=VMEM,
        out_shape=jax.ShapeDtypeStruct((128, 2, HEAD), jnp.float32),
        compiler_params=SMALL_VMEM,
        name="line_stats",
    )(gradient)


def update_kernel(where_ref, stats_ref, gradient_ref, master_ref, moment_ref, own_master_ref, own_moment_ref,
                  heads_ref, neurons_ref, params_ref, new_master_ref, new_moment_ref, new_heads_ref, new_neurons_ref):
    x, own = where_ref[0], where_ref[1]
    column = jnp.sum(jnp.sum(stats_ref[...], axis=0), axis=0)
    total = jnp.sum(column[0:1], axis=1, keepdims=True) + column[1:2]
    mine = jnp.sum(stats_ref[:, x], axis=0)
    neuron_sq, head_sq = mine[0:1], mine[1:2]
    clip = jnp.minimum(1.0, 256.0 / (jnp.sqrt(total) + 1e-06))
    new_heads = 0.95 * heads_ref[...] + 0.05 * clip * clip * head_sq / (DIN * HEAD)
    new_neurons = 0.95 * neurons_ref[...] + 0.05 * clip * clip * neuron_sq / DIN
    new_heads_ref[...] = new_heads
    new_neurons_ref[...] = new_neurons
    for p, second in ((0, new_heads), (1, new_neurons)):
        denom = jnp.sqrt(second / SECOND_FIX) + 1e-08

        def step(master, moment, gradient):
            new_moment = 0.9 * moment + 0.1 * clip * gradient
            update = new_moment / FIRST_FIX / denom
            return new_moment, master - 0.01 * (update + 0.1 * master)

        new_moment_ref[p], new_master_ref[p] = step(own_master_ref[p], own_moment_ref[p], gradient_ref[own, p])
        for k in range(8):
            _, new_master = step(master_ref[k, p], moment_ref[k, p], gradient_ref[k, p])
            params_ref[k, p] = new_master.astype(jnp.bfloat16)


def update_of(where, stats, gradient, master, moment, own_master, own_moment, heads, neurons):
    own = jax.ShapeDtypeStruct((2, ROWS, HEAD), jnp.float32)
    row = jax.ShapeDtypeStruct((1, HEAD), jnp.float32)
    return pl.pallas_call(
        update_kernel,
        in_specs=[SMEM] + [VMEM] * 8,
        out_specs=[VMEM] * 5,
        out_shape=[jax.ShapeDtypeStruct((8, 2, ROWS, HEAD), jnp.bfloat16), own, own, row, row],
        compiler_params=SMALL_VMEM,
        name="update",
    )(where, stats, gradient, master, moment, own_master, own_moment, heads, neurons)


def place_kernel(slot_ref, plane_ref, *rest):
    out_ref, sems = rest[-2:]
    slot = slot_ref[0]

    def copies(k):
        for hi in range(8):
            for p in range(2):
                source = plane_ref.at[hi, :, p] if k == 0 else plane_ref.at[:, hi, p]
                yield pltpu.make_async_copy(source, out_ref.at[p, hi, :, k], sems.at[hi, p])

    for k in range(2):

        @pl.when(slot == k)
        def _():
            for copy in copies(k):
                copy.start()
            for copy in copies(k):
                copy.wait()


def place(slot, plane, before, name):
    before = () if before is None else (before,)
    return pl.pallas_call(
        place_kernel,
        in_specs=[SMEM, VMEM] + [HBM] * len(before),
        out_specs=HBM,
        out_shape=jax.ShapeDtypeStruct((2, 8, 8, 2, ROWS, HEAD), jnp.bfloat16),
        scratch_shapes=[pltpu.SemaphoreType.DMA((8, 2))],
        input_output_aliases={2: 0} if before else {},
        compiler_params=SMALL_VMEM,
        name=name,
    )(slot, plane, *before)


def on_device(grads, master, moment, v_heads, v_neurons):
    c = lax.axis_index("c")
    x = lax.axis_index("x")
    own = jnp.where(c == 0, lax.axis_index("y"), lax.axis_index("z"))

    where = jnp.stack([x, own]).astype(jnp.int32)
    core = c.reshape(1).astype(jnp.int32)
    halves = grads[0].reshape(2, 64, 2, ROWS, HEAD)
    theirs = lax.dynamic_index_in_dim(halves, 1 - c, 2, keepdims=False)
    halves, theirs = lax.optimization_barrier((halves, theirs))
    mine = lax.dynamic_index_in_dim(halves, c, 2, keepdims=False)
    power_a, power_o = power_of(master, (0, 1)), power_of(moment, (0, 1))
    state = jnp.concatenate(in_two(master, power_a) + in_two(moment, power_o), axis=0)
    heads = jnp.broadcast_to(v_heads, (1, HEAD))
    neurons = v_neurons.reshape(1, HEAD)
    sums = mine.astype(jnp.float32) + swap_cores(theirs).astype(jnp.float32)
    power = power_of(sums, None)
    sums = sums.reshape(2, 8, 8, ROWS, HEAD)
    ordered = jnp.where(c == 0, sums.transpose(1, 2, 0, 3, 4), sums.transpose(2, 1, 0, 3, 4))
    message = jnp.concatenate(
        [as_half(ordered, power).reshape(8, 512, HEAD), jnp.full((8, 8, HEAD), power, jnp.float16)], axis=1
    )
    first_row, powers = row_at(0, 1.0), row_at(1, power_a) + row_at(2, power_o)
    message, state, first_row, powers, where, core, heads = lax.optimization_barrier(
        (message, state, first_row, powers, where, core, heads)
    )
    got = exchange(message, DP, FIRST)
    partial = jnp.sum(got[:, :512].astype(jnp.float32) * scale_at(got, 512)[:, None, :], axis=0)

    power = power_of(partial, 0)
    message = jnp.concatenate([as_half(partial, power), state, (powers + power * first_row).astype(jnp.float16)], axis=0)
    message = lax.optimization_barrier(message)
    got = exchange(jnp.broadcast_to(message, (8, *message.shape)), DP, SECOND)
    gradient = jnp.sum(got[:, :512].astype(jnp.float32) * scale_at(got, 768)[:, None, :], axis=0) / 128.0
    gradient = gradient.reshape(8, 2, ROWS, HEAD)
    line_master = out_of_two(got[:, 512:576], got[:, 576:640], scale_at(got, 769)).reshape(8, 2, ROWS, HEAD)
    line_moment = out_of_two(got[:, 640:704], got[:, 704:768], scale_at(got, 770)).reshape(8, 2, ROWS, HEAD)
    stats, line_master, line_moment = lax.optimization_barrier((line_stats(gradient), line_master, line_moment))
    stats = exchange(stats, (*DP, "x"), STATS)
    params, new_master, new_moment, new_heads, new_neurons = update_of(
        where, stats.reshape(16, NX, 2, HEAD), gradient, line_master, line_moment, master, moment, heads, neurons
    )
    plane = exchange(jnp.broadcast_to(params.reshape(512, HEAD), (8, 512, HEAD)), DP, FIRST)
    plane = plane.reshape(8, 8, 2, ROWS, HEAD)
    other = swap_cores(plane)
    params = place(core, plane, None, "place_mine")
    params = place(1 - core, other, params, "place_theirs").reshape(2, DIN, HEAD)
    return (params, new_master, new_moment, new_heads[0, :1], new_neurons.reshape(HEAD))


def solution(mesh):
    split = Mesh(mesh.devices.reshape(NZ, NY, NC, NX), ("z", "y", "c", "x"))
    return jax.shard_map(
        on_device,
        mesh=split,
        in_specs=(
            P(DP, None, None, "x"),
            P(None, DP, "x"),
            P(None, DP, "x"),
            P("x"),
            P("x"),
        ),
        out_specs=(
            P(None, None, "x"),
            P(None, DP, "x"),
            P(None, DP, "x"),
            P("x"),
            P("x"),
        ),
        check_vma=False,
    )
```
